32 devices in a mesh: gx: 4 (over x, core), gy: 8 (over z, y).
Axes of the slice: x: 2, y: 2, z: 4, core: 2. Of those that a mesh axis runs over, the one named last changes fastest.
Arguments:
- base: int32 [2, 3, 65536], P(None, None, ('gx', 'gy')), may hold values from -2 to 125, as said below
- offset: float32 [2, 3, 65536], P(None, None, ('gx', 'gy')), may hold values from 0.5 to 1.5
- velocity: float32 [3, 65536], P(None, ('gx', 'gy')), may hold values from -4 to 4
- affine: float32 [9, 65536], P(None, ('gx', 'gy')), may hold values from -3 to 3
- volume: float32 [65536], P(('gx', 'gy')), may hold values from 0.8 to 1.25
- node_mask: int32 [128, 128, 128], P('gx', 'gy'), may hold values 0 or 1
- direction: int32 [65536], P(('gx', 'gy')), may hold values from 0 to 8, as said below
Outputs:
- migrated: float32 [16, 98304], P(None, ('gx', 'gy'))
The draws below stay inside these ranges and needn't reach their ends.
Inputs may be any that keep to these rules, and one draw needn't show every extreme that they name: base[s, 0] lies in -2 to 31, base[s, 1] in -2 to 15, base[s, 2] in 0 to 125. Of one block column's rows, at most 128 carry any one direction other than 4; in every draw some block column has exactly 128 rows in some direction.
All inputs are finite; a program needn't handle non-finite values. No bound on the sum of `node_mask` on one device may be relied on, other than what follows from the above.
Results may differ from the reference program's by a relative error of at most 0.0003.
Values may be sent and summed in bfloat16 or wider, within the bound.
A program may use at most 64 MiB of HBM per device.

```python
import jax
import jax.numpy as jnp

CX = 32
CY = 16
NZ = 128
PART_DEV = 2048
CAP = 128
NX = 128
NY = 128
NPART = 65536
N_GX = 4
N_GY = 8


def draw_base(key, part):
    key_x, key_y, key_z = jax.random.split(key, 3)
    first = jax.random.randint(key_x, (2, 1, NPART), -2, CX)
    second = jax.random.randint(key_y, (2, 1, NPART), -2, CY)
    third = jax.random.randint(key_z, (2, 1, NPART), 0, NZ - 2)
    return jnp.concatenate([first, second, third], 1).astype(jnp.int32)


def draw_direction(key, part):
    groups = NPART // PART_DEV
    keys = jax.random.split(jax.random.fold_in(key, 17), 4)
    level = jax.random.randint(keys[0], (groups, 1), 1, 4)
    raw = jnp.minimum(jax.random.randint(keys[1], (groups, 8), 0, CAP // 3 + 1) * level, CAP)
    chosen = jax.random.randint(keys[2], (groups, 1), 0, 8)
    counts = jnp.where(jnp.arange(8)[None, :] == chosen, CAP, raw)
    bounds = jnp.cumsum(counts, 1)
    order = jax.vmap(lambda subkey: jax.random.permutation(subkey, PART_DEV))(jax.random.split(keys[3], groups))
    lane = jnp.sum((order[:, :, None] >= bounds[:, None, :]).astype(jnp.int32), 2)
    code = jnp.where(lane < 4, lane, jnp.where(lane < 8, lane + 1, 4))
    return code.reshape(NPART).astype(jnp.int32)


def set_ends(drawn, own_key, least, largest):
    shape = drawn.shape
    spot = [jax.random.randint(jax.random.fold_in(own_key, axis), (), 0, shape[axis]) for axis in range(len(shape))]
    drawn = drawn.at[tuple(spot)].set(least)
    longest = shape.index(max(shape))
    spot[longest] = (spot[longest] + 1) % shape[longest]
    return drawn.at[tuple(spot)].set(largest)


def block_levels(own_key, shape, cuts, smallest, high):
    def one(dim, shards_of):
        steps = jax.random.uniform(jax.random.fold_in(jax.random.fold_in(own_key, 6), dim), (shards_of,), jnp.float32, smallest / len(cuts), high / len(cuts))
        return jnp.repeat(jnp.exp(steps), shape[dim] // shards_of).reshape((-1,) + (1,) * (len(shape) - dim - 1))

    loudness = one(*cuts[0])
    for cut in cuts[1:]:
        loudness = loudness * one(*cut)
    return loudness


def scatter_about(rng, shape, scale, limit, shards=(), held_as=jnp.bfloat16):
    entries = jax.random.normal(rng, shape, jnp.float32) * scale
    if len(shards) > 0:
        entries = block_levels(rng, shape, shards, -0.22, 0.18) * entries
    return jnp.clip(entries, min=-limit, max=limit).astype(held_as)


def setup_inputs(seed: int = 0) -> dict:
    streams_of = jax.random.split(jax.random.key(seed), 8)
    base = draw_base(jax.random.fold_in(streams_of[7], 71), 0)
    offset = jnp.clip(0.5 + 1.0 * jax.random.uniform(streams_of[1], (2, 3, NPART), jnp.float32) ** block_levels(streams_of[1], (2, 3, NPART), ((2, 32),), -0.2, 0.2), 0.5, 1.5)
    velocity = scatter_about(streams_of[2], (3, NPART), 1.0, 4.0, ((1, 32),), jnp.float32)
    affine = scatter_about(streams_of[3], (9, NPART), 0.5, 3.0, ((1, 32),), jnp.float32)
    volume = jnp.clip(0.8 + 0.45 * jax.random.uniform(streams_of[4], (NPART,), jnp.float32) ** block_levels(streams_of[4], (NPART,), ((0, 32),), -0.2, 0.2), 0.8, 1.25)
    node_mask = set_ends((jax.random.randint(streams_of[5], (NX, NY, NZ), 0, 6) < 1).astype(jnp.int32), jax.random.fold_in(streams_of[5], 1), 0, 1)
    direction = draw_direction(jax.random.fold_in(streams_of[7], 71), 0)
    return {"base": base, "offset": offset, "velocity": velocity, "affine": affine, "volume": volume, "node_mask": node_mask, "direction": direction}


PARTICLE_MASS = 1.0
STIFFNESS = 4.0
TIME_STEP = 0.1
GRAVITY = 3.0
MASS_FLOOR = 0.5


def rounded(value):
    return value.astype(jnp.bfloat16).astype(jnp.float32)


def spline(frac):
    return [0.5 * (1.5 - frac) ** 2, 0.75 - (frac - 1.0) ** 2, 0.5 * (frac - 0.5) ** 2]


def substep(bases, offsets, velocity, affine, volume, keep, block_x, block_y):
    count = velocity.shape[1]
    start_x = (bases[0] + block_x * CX + 2).astype(jnp.int32)
    start_y = (bases[1] + block_y * CY + 2).astype(jnp.int32)
    start_z = bases[2].astype(jnp.int32)
    weights = [spline(offsets[axis]) for axis in range(3)]
    slopes = [[weights[axis][node] * (node - offsets[axis]) for node in range(3)] for axis in range(3)]
    stress = -STIFFNESS * (volume - 1.0)
    matrix = PARTICLE_MASS * affine.reshape(3, 3, count) + stress[None, None] * jnp.eye(3, dtype=jnp.float32)[:, :, None]
    zero_row = jnp.zeros((1, count), jnp.float32)
    moment = jnp.concatenate([PARTICLE_MASS * jnp.ones((1, count), jnp.float32), PARTICLE_MASS * velocity], 0)
    along = [jnp.concatenate([zero_row, matrix[:, axis]], 0) for axis in range(3)]
    grid = jnp.zeros((4, NX + 4, NY + 4, NZ), jnp.float32)
    for node_x in range(3):
        for node_y in range(3):
            plain = rounded(weights[0][node_x] * weights[1][node_y])
            slope_x = rounded(slopes[0][node_x] * weights[1][node_y])
            slope_y = rounded(weights[0][node_x] * slopes[1][node_y])
            for node_z in range(3):
                first = rounded(weights[2][node_z] * moment + slopes[2][node_z] * along[2])
                second = rounded(weights[2][node_z] * along[0])
                third = rounded(weights[2][node_z] * along[1])
                values = plain * first + slope_x * second + slope_y * third
                grid = grid.at[:, start_x + node_x, start_y + node_y, start_z + node_z].add(values)
    inner = grid[:, 2:NX + 2, 2:NY + 2]
    speed = inner[1:4] / jnp.maximum(inner[0], MASS_FLOOR)[None]
    speed = speed.at[2].add(-TIME_STEP * GRAVITY)
    speed = (speed * keep[None]).astype(jnp.bfloat16)
    padded = jnp.pad(speed, ((0, 0), (2, 2), (2, 2), (0, 0))).astype(jnp.float32)
    new_velocity = jnp.zeros((3, count), jnp.float32)
    part_x = jnp.zeros((3, count), jnp.float32)
    part_y = jnp.zeros((3, count), jnp.float32)
    part_z = jnp.zeros((3, count), jnp.float32)
    for node_x in range(3):
        for node_y in range(3):
            plain = rounded(weights[0][node_x] * weights[1][node_y])
            slope_x = rounded(slopes[0][node_x] * weights[1][node_y])
            slope_y = rounded(weights[0][node_x] * slopes[1][node_y])
            for node_z in range(3):
                nodal = padded[:, start_x + node_x, start_y + node_y, start_z + node_z]
                new_velocity = new_velocity + plain * nodal * weights[2][node_z]
                part_x = part_x + slope_x * nodal * weights[2][node_z]
                part_y = part_y + slope_y * nodal * weights[2][node_z]
                part_z = part_z + plain * nodal * slopes[2][node_z]
    new_affine = 4.0 * jnp.stack([part_x, part_y, part_z], 1).reshape(9, count)
    new_volume = volume * (1.0 + TIME_STEP * (new_affine[0] + new_affine[4] + new_affine[8]))
    return new_velocity, new_affine, new_volume


def reference(base, offset, velocity, affine, volume, node_mask, direction):
    devices = N_GX * N_GY
    count = velocity.shape[1]
    owner = (jnp.arange(count) // PART_DEV).astype(jnp.int32)
    block_x = owner // N_GY
    block_y = owner % N_GY
    keep = (1 - node_mask).astype(jnp.float32)
    state_v, state_c, state_j = velocity, affine, volume
    for sub in range(2):
        state_v, state_c, state_j = substep(base[sub], offset[sub], state_v, state_c, state_j, keep, block_x, block_y)
    position = base[1].astype(jnp.float32) + offset[1] + TIME_STEP * state_v
    step_x = direction // 3 - 1
    step_y = direction % 3 - 1
    inside = (block_x + step_x >= 0) & (block_x + step_x < N_GX) & (block_y + step_y >= 0) & (block_y + step_y < N_GY)
    moving = jnp.where(inside, direction, 4).astype(jnp.int32)
    step_x = jnp.where(inside, step_x, 0)
    step_y = jnp.where(inside, step_y, 0)
    shift_rows = jnp.stack([step_x * CX, step_y * CY, jnp.zeros_like(step_x)]).astype(jnp.float32)
    state = jnp.concatenate([position - shift_rows, state_v, state_c, state_j[None]], 0)
    lane = jnp.where(moving < 4, moving, moving - 1)
    hits = (jnp.arange(8, dtype=jnp.int32)[:, None] == lane[None]) & (moving != 4)[None]
    running = jnp.cumsum(hits.astype(jnp.int32).reshape(8, devices, PART_DEV), 2).reshape(8, count) - 1
    rank = jnp.sum(jnp.where(hits, running, 0), 0).astype(jnp.int32)
    width = PART_DEV + 8 * CAP
    target = (block_x + step_x) * N_GY + (block_y + step_y)
    local_row = (jnp.arange(count) % PART_DEV).astype(jnp.int32)
    slot = jnp.where(moving == 4, owner * width + local_row, target * width + PART_DEV + lane * CAP + rank).astype(jnp.int32)
    migrated = jnp.zeros((16, devices * width), jnp.float32).at[:, slot].set(state)
    return migrated
```

```python
import functools

import jax
import jax.numpy as jnp
from jax import lax
from jax.experimental import pallas as pl
from jax.experimental.pallas import tpu as pltpu
from jax.sharding import PartitionSpec as P

PARTICLE_MASS = 1.0
STIFFNESS = 4.0
TIME_STEP = 0.1
GRAVITY = 3.0
MASS_FLOOR = 0.5
LANES = 128
OUTSIDE = -100

F32 = jnp.float32
BF16 = jnp.bfloat16
NT = (((1,), (1,)), ((), ()))

SIDES = ((0, -1), (0, 1), (-1, 0), (1, 0))
CORNERS = ((-1, -1), (-1, 1), (1, -1), (1, 1))
BLOCKS = SIDES + CORNERS
ISSUE = (4, 5, 6, 7, 0, 1, 2, 3)
CORNER_ROWS = 16


class Sizes:
    def __init__(self, size_x, size_y, depth, rows, chunk):
        self.x, self.y, self.depth, self.rows, self.chunk = size_x, size_y, depth, rows, chunk
        self.steps = rows // chunk
        self.cells = size_x * size_y
        counts = [2 * size_x] * 2 + [2 * size_y] * 2
        self.sides = [(sum(counts[:k]), counts[k]) for k in range(4)]
        self.corner = sum(counts)
        self.used = self.corner + 16
        self.edge = -(-self.used // 256) * 256


def spline(frac):
    return [0.5 * (1.5 - frac) ** 2, 0.75 - (frac - 1.0) ** 2, 0.5 * (frac - 0.5) ** 2]


def pick(place, values):
    return jnp.where(
        place == 0,
        values[0],
        jnp.where(place == 1, values[1], jnp.where(place == 2, values[2], 0.0)),
    )


def weights_of(offsets):
    weights = [spline(offsets[axis : axis + 1]) for axis in range(3)]
    slopes = [
        [weights[axis][node] * (float(node) - offsets[axis : axis + 1]) for node in range(3)]
        for axis in range(3)
    ]
    return (weights, slopes)


def rows_iota(count):
    return lax.broadcasted_iota(jnp.int32, (count, 1), 0)


def build(sz, bases, offsets, tab, tables, depth_w, depth_s):
    xw, xs, yw, ys = tables
    width = bases.shape[1]
    weights, slopes = weights_of(offsets)
    from_x = bases[0:1] + 2
    from_y = bases[1:2] + 2
    edge = rows_iota(8)
    for size, start, axis, plain, slope in ((sz.x, from_x, 0, xw, xs), (sz.y, from_y, 1, yw, ys)):
        place = rows_iota(size) + 2 - start
        plain[0:size] = pick(place, weights[axis])
        slope[0:size] = pick(place, slopes[axis])
        coord = jnp.where(edge < 2, edge, jnp.where(edge < 4, edge + size, OUTSIDE))
        place = coord - start
        plain[size : size + 8] = pick(place, weights[axis])
        slope[size : size + 8] = pick(place, slopes[axis])

    def put(row, count, wx, sx, wy, sy):
        tab[row : row + count, 0:width] = (wx * wy).astype(BF16)
        tab[row : row + count, width : 2 * width] = (sx * wy).astype(BF16)
        tab[row : row + count, 2 * width : 3 * width] = (wx * sy).astype(BF16)

    wide_w, wide_s = (xw[0 : sz.x], xs[0 : sz.x])
    tall_w, tall_s = (yw[0 : sz.y], ys[0 : sz.y])
    for k in range(4):
        one = slice(sz.y + k, sz.y + k + 1)
        put(k * sz.x, sz.x, wide_w, wide_s, yw[one], ys[one])
    for k in range(4):
        one = slice(sz.x + k, sz.x + k + 1)
        put(sz.sides[2][0] + k * sz.y, sz.y, xw[one], xs[one], tall_w, tall_s)
    spot = rows_iota(16)
    coord_x = ((spot >> 1) & 1) + (spot >> 3) * (sz.x + 2)
    coord_y = (spot & 1) + ((spot >> 2) & 1) * (sz.y + 2)
    place_x = coord_x - from_x
    place_y = coord_y - from_y
    put(
        sz.corner,
        16,
        pick(place_x, weights[0]),
        pick(place_x, slopes[0]),
        pick(place_y, weights[1]),
        pick(place_y, slopes[1]),
    )
    for y in range(sz.y):
        one = slice(y, y + 1)
        put(sz.edge + y * sz.x, sz.x, wide_w, wide_s, yw[one], ys[one])
    place = rows_iota(sz.depth) - bases[2:3]
    depth_w[...] = pick(place, weights[2])
    depth_s[...] = pick(place, slopes[2])


def build_right(sz, vel, aff, vol, depth_w, depth_s, right):
    depth = sz.depth
    width = vol.shape[1]
    stress = -STIFFNESS * (vol - 1.0)

    def entry(i, j):
        value = PARTICLE_MASS * aff[3 * i + j]
        return value + stress if i == j else value

    plain = depth_w[...]
    slope = depth_s[...]
    right[0:depth, 0:width] = (plain * PARTICLE_MASS).astype(BF16)
    for i in range(3):
        rows = slice((i + 1) * depth, (i + 2) * depth)
        moment = PARTICLE_MASS * vel[i]
        right[rows, 0:width] = (plain * moment + slope * entry(i, 2)).astype(BF16)
        right[rows, width : 2 * width] = (plain * entry(i, 0)).astype(BF16)
        right[rows, 2 * width : 3 * width] = (plain * entry(i, 1)).astype(BF16)


def reduce_depth(sz, result, depth_w, depth_s):
    width = depth_w.shape[1]

    def fold(value):
        return jnp.sum(value.reshape(sz.depth // 8, 8, width), 0)

    sums = []
    for i in range(3):
        rows = slice(i * sz.depth, (i + 1) * sz.depth)
        plain = result[rows, 0:width]
        sums.append(fold(plain * depth_w[...]))
        sums.append(fold(result[rows, width : 2 * width] * depth_w[...]))
        sums.append(fold(result[rows, 2 * width : 3 * width] * depth_w[...]))
        sums.append(fold(plain * depth_s[...]))
    return sums


def finish(sums, vol):
    vel = [jnp.sum(sums[4 * i], 0, keepdims=True) for i in range(3)]
    aff = [
        4.0 * jnp.sum(sums[4 * i + 1 + a], 0, keepdims=True) for i in range(3) for a in range(3)
    ]
    return (vel, aff, vol * (1.0 + TIME_STEP * (aff[0] + aff[4] + aff[8])))


def neighbour(counts, dx, dy):
    to_x = lax.axis_index("gx") + dx
    to_y = lax.axis_index("gy") + dy
    exists = (to_x >= 0) & (to_x < counts[0]) & (to_y >= 0) & (to_y < counts[1])
    return (exists, {"gx": to_x, "gy": to_y})


def greet(counts):
    barrier = pltpu.get_barrier_semaphore()
    for dx, dy in BLOCKS:
        exists, where = neighbour(counts, dx, dy)

        @pl.when(exists)
        def _():
            pl.semaphore_signal(
                barrier, inc=1, device_id=where, device_id_type=pl.DeviceIdType.MESH
            )


def await_peers(counts):
    barrier = pltpu.get_barrier_semaphore()
    peers = 0
    for dx, dy in BLOCKS:
        exists, _ = neighbour(counts, dx, dy)
        peers = peers + exists.astype(jnp.int32)
    pl.semaphore_wait(barrier, peers)


def transfers(counts, sign, source, target, send_sems, recv_sems):
    copies = []
    for k, (dx, dy) in enumerate(BLOCKS):
        exists, where = neighbour(counts, sign * dx, sign * dy)
        copy = pltpu.make_async_remote_copy(
            src_ref=source(k),
            dst_ref=target(k),
            send_sem=send_sems.at[k],
            recv_sem=recv_sems.at[k],
            device_id=where,
            device_id_type=pl.DeviceIdType.MESH,
        )
        comes, _ = neighbour(counts, -sign * dx, -sign * dy)
        copies.append((exists, comes, copy))
    return copies


def start_all(copies, picked=ISSUE):
    for k in picked:
        pl.when(copies[k][0])(copies[k][2].start)


def wait_arrivals(copies, picked=ISSUE):
    for k in picked:
        pl.when(copies[k][1])(copies[k][2].wait_recv)


def wait_sends(copies):
    for exists, _, copy in copies:
        pl.when(exists)(copy.wait_send)


def clear_missing(counts, sign, target):
    for k, (dx, dy) in enumerate(BLOCKS):
        comes, _ = neighbour(counts, -sign * dx, -sign * dy)

        @pl.when(jnp.logical_not(comes))
        def _():
            view = target(k)
            view[...] = jnp.zeros(view.shape, view.dtype)


def edge_views(sz, sides, tiles):
    def view(k):
        if k < 4:
            return sides.at[pl.ds(*sz.sides[k])]
        return tiles.at[pl.ds((k - 4) * CORNER_ROWS, CORNER_ROWS)]

    return view


def kernel(sz, counts, capacity, base, offset, vel, aff, vol, mask, direction, out, *scratch):
    (
        tabs, right, depth_w, depth_s, result, inner_sums, edge_total, total, speed, keep, wide, wide_edge,
        ratio, chosen, slots, packed, xw, xs, yw, ys,
        margins, corners, got, got_corners, sent, sent_corners, halo, halo_corners, spread,
        buckets, arrived, send_sems, recv_sems, bucket_sends, bucket_recvs,
    ) = scratch
    size_x, size_y, depth = sz.x, sz.y, sz.depth
    width = sz.chunk
    tables = (xw, xs, yw, ys)
    greet(counts)

    margin_copies, halo_copies = ([], [])
    for s in range(2):
        arriving = edge_views(sz, got.at[s], got_corners.at[s])
        clear_missing(counts, 1, arriving)
        margin_copies.append(
            transfers(
                counts, 1, edge_views(sz, margins.at[s], corners.at[s]), arriving,
                send_sems.at[2 * s], recv_sems.at[2 * s],
            )
        )
        arriving = edge_views(sz, halo.at[s], halo_corners.at[s])
        clear_missing(counts, -1, arriving)
        halo_copies.append(
            transfers(
                counts, -1, edge_views(sz, sent.at[s], sent_corners.at[s]), arriving,
                send_sems.at[2 * s + 1], recv_sems.at[2 * s + 1],
            )
        )
    order = [0, 1, 2, 3, 5, 6, 7, 8]
    slot_of = [order.index(3 * (dx + 1) + dy + 1) for dx, dy in BLOCKS]
    clear_missing(counts, 1, lambda k: arrived.at[slot_of[k]])
    bucket_copies = transfers(
        counts, 1, lambda k: buckets.at[slot_of[k]], lambda k: arrived.at[slot_of[k]],
        bucket_sends, bucket_recvs,
    )
    for step in range(sz.steps):
        right[step, 0:depth, width : 3 * width] = jnp.zeros((depth, 2 * width), BF16)
        for s in range(2):
            tabs[s, step, sz.used : sz.edge] = jnp.zeros((sz.edge - sz.used, 3 * width), BF16)
    for y in range(size_y):
        column = mask[pl.ds(y, size_x, stride=size_y), :]
        keep[y * size_x : (y + 1) * size_x] = (1 - column).astype(F32)

    def lanes_of(step):
        return pl.ds(pl.multiple_of(step * width, width), width)

    def prepare(s, step):
        lanes = lanes_of(step)
        build(
            sz, base[:, s, lanes], offset[:, s, lanes], tabs.at[s, step], tables,
            depth_w.at[s, :, lanes], depth_s.at[s, :, lanes],
        )

    def scatter_edge(s, step):
        edge_total[...] += lax.dot_general(
            tabs[s, step, 0 : sz.used], right[step], NT, preferred_element_type=F32
        )

    def scatter_inner(s, step):
        added = lax.dot_general(
            tabs[s, step, sz.edge :], right[step], NT, preferred_element_type=F32
        )
        for c in range(4):
            total[c] += added[:, c * depth : (c + 1) * depth]

    def send_margins(s):
        margins[s] = edge_total[0 : sz.corner].astype(BF16)
        for k in range(4):
            for c in range(4):
                spread[k * 16 + 4 * c : k * 16 + 4 * c + 4, :] = edge_total[
                    sz.corner + 4 * k : sz.corner + 4 * k + 4, c * depth : (c + 1) * depth
                ]
        corners[s] = spread[...].astype(BF16)
        start_all(margin_copies[s])

    def add_margins(s):
        wait_arrivals(margin_copies[s])
        for k, low in ((1, 0), (0, sz.cells - 2 * size_x)):
            start, count = sz.sides[k]
            for c in range(4):
                block = got[s, start : start + count, c * depth : (c + 1) * depth]
                total[c, low : low + count] += block.astype(F32)
        for k, low in ((2, size_x - 2), (3, 0)):
            start = sz.sides[k][0]
            block = got[s, start : start + 2 * size_y].astype(F32)
            for i in range(2):
                rows = pl.ds(low + i, size_y, stride=size_x)
                for c in range(4):
                    lanes = slice(c * depth, (c + 1) * depth)
                    total[c, rows] += block[i * size_y : (i + 1) * size_y, lanes]
        spread[...] = got_corners[s].astype(F32)
        for k, (dx, dy) in enumerate(CORNERS):
            low_x = size_x - 2 if dx < 0 else 0
            low_y = size_y - 2 if dy < 0 else 0
            for i in range(2):
                for j in range(2):
                    row = (low_y + j) * size_x + low_x + i
                    for c in range(4):
                        here = k * 16 + 4 * c + 2 * i + j
                        total[c, row : row + 1] += spread[here : here + 1]

    def velocities():
        mass = jnp.maximum(total[0], MASS_FLOOR)
        for axis in range(3):
            value = total[axis + 1] / mass
            if axis == 2:
                value = value - TIME_STEP * GRAVITY
            speed[axis] = value * keep[...]

    def send_halo(s):
        for k, low in ((1, 0), (0, sz.cells - 2 * size_x)):
            start, count = sz.sides[k]
            for c in range(3):
                lanes = slice(c * depth, (c + 1) * depth)
                sent[s, start : start + count, lanes] = speed[c, low : low + count].astype(BF16)
        for k, low in ((2, size_x - 2), (3, 0)):
            for i in range(2):
                start = sz.sides[k][0] + i * size_y
                rows = pl.ds(low + i, size_y, stride=size_x)
                for c in range(3):
                    lanes = slice(c * depth, (c + 1) * depth)
                    sent[s, start : start + size_y, lanes] = speed[c, rows].astype(BF16)
        for k, (dx, dy) in enumerate(CORNERS):
            low_x = size_x - 2 if dx < 0 else 0
            low_y = size_y - 2 if dy < 0 else 0
            for i in range(2):
                for j in range(2):
                    row = (low_y + j) * size_x + low_x + i
                    for c in range(3):
                        here = k * 16 + 4 * c + 2 * i + j
                        spread[here : here + 1] = speed[c, row : row + 1]
        sent_corners[s] = spread[...].astype(BF16)
        start_all(halo_copies[s])

    def fill_wide():
        for c in range(3):
            wide[c * depth : (c + 1) * depth, :] = speed[c].T.astype(BF16)

    def fill_wide_edge(s):
        wait_arrivals(halo_copies[s])
        spread[...] = halo_corners[s].astype(F32)
        for c in range(3):
            lanes = slice(c * depth, (c + 1) * depth)
            tiles = [spread[k * 16 + 4 * c : k * 16 + 4 * c + 4] for k in range(4)]
            rest = jnp.zeros((sz.edge - sz.used, depth), F32)
            outer = jnp.concatenate([halo[s, :, lanes].astype(F32)] + tiles + [rest], 0)
            wide_edge[lanes, :] = outer.T.astype(BF16)

    def gather_inner(s, step):
        lanes = lanes_of(step)
        result[...] = jnp.dot(wide[...], tabs[s, step, sz.edge :], preferred_element_type=F32)
        sums = reduce_depth(sz, result, depth_w.at[s, :, lanes], depth_s.at[s, :, lanes])
        for k in range(12):
            inner_sums[k, :, lanes] = sums[k]

    def gather_edge(s, step, volume):
        lanes = lanes_of(step)
        result[...] = jnp.dot(wide_edge[...], tabs[s, step, 0 : sz.edge], preferred_element_type=F32)
        sums = reduce_depth(sz, result, depth_w.at[s, :, lanes], depth_s.at[s, :, lanes])
        return finish([sums[k] + inner_sums[k, :, lanes] for k in range(12)], volume)

    def loop(body):
        lax.fori_loop(0, sz.steps, lambda step, carry: (body(step), carry)[1], 0)

    def rows_of(ref, lanes, count):
        return [ref[k : k + 1, lanes] for k in range(count)]

    edge_total[...] = jnp.zeros_like(edge_total)
    total[...] = jnp.zeros_like(total)

    def first(step):
        lanes = lanes_of(step)
        prepare(0, step)
        build_right(
            sz, rows_of(vel, lanes, 3), rows_of(aff, lanes, 9), vol[:, lanes],
            depth_w.at[0, :, lanes], depth_s.at[0, :, lanes], right.at[step],
        )
        scatter_edge(0, step)

    def first_inner(step):
        scatter_inner(0, step)
        prepare(1, step)

    def second(step):
        lanes = lanes_of(step)
        new_vel, new_aff, new_vol = gather_edge(0, step, vol[:, lanes])
        ratio[:, lanes] = new_vol
        build_right(
            sz, new_vel, new_aff, new_vol, depth_w.at[1, :, lanes], depth_s.at[1, :, lanes],
            right.at[step],
        )
        scatter_edge(1, step)

    index_x = lax.axis_index("gx")
    index_y = lax.axis_index("gy")

    def route(code):
        step_x = jnp.where(code < 3, -1, jnp.where(code > 5, 1, 0))
        step_y = code - 3 * step_x - 4
        to_x = step_x + index_x
        to_y = step_y + index_y
        inside = (to_x >= 0) & (to_x < counts[0]) & (to_y >= 0) & (to_y < counts[1])
        return (
            jnp.where(inside, code, 4),
            jnp.where(inside, step_x, 0),
            jnp.where(inside, step_y, 0),
        )

    def rank_rows():
        parts = sz.rows // LANES
        place = rows_iota(8)
        codes = jnp.where(place < 4, place, place + 1)
        hits = []
        for part in range(parts):
            moving, _, _ = route(direction[:, part * LANES : (part + 1) * LANES])
            hits.append(jnp.where(moving == codes, 1.0, 0.0))
        above = lax.broadcasted_iota(jnp.int32, (LANES, 2 * LANES), 0)
        along = lax.broadcasted_iota(jnp.int32, (LANES, 2 * LANES), 1)
        summer = jnp.where(above <= along, 1.0, 0.0).astype(BF16)
        sums = jnp.dot(
            jnp.concatenate(hits, 0).astype(BF16), summer, preferred_element_type=F32
        )
        before = jnp.broadcast_to((place * capacity).astype(F32), (8, LANES))
        for part in range(parts):
            mine = slice(part * 8, (part + 1) * 8)
            slot = jnp.sum(hits[part] * (sums[mine, 0:LANES] + before), 0, keepdims=True) - 1.0
            slots[:, part * LANES : (part + 1) * LANES] = slot.astype(jnp.int32)
            before = before + sums[mine, LANES:]

    def second_inner(step):
        lanes = lanes_of(step)
        scatter_inner(1, step)
        slot = slots[:, lanes]
        for k in range(8):
            here = slot - k * capacity == rows_iota(capacity)
            chosen[k * capacity : (k + 1) * capacity, lanes] = jnp.where(here, 1.0, 0.0).astype(BF16)

    def last(step):
        lanes = lanes_of(step)
        new_vel, new_aff, new_vol = gather_edge(1, step, ratio[:, lanes])
        moving, step_x, step_y = route(direction[:, lanes])
        shift = (step_x * size_x, step_y * size_y, None)
        bases = base[:, 1, lanes]
        offsets = offset[:, 1, lanes]
        spots = []
        for axis in range(3):
            spot = bases[axis : axis + 1].astype(F32) + offsets[axis : axis + 1]
            spot = spot + TIME_STEP * new_vel[axis]
            if shift[axis] is not None:
                spot = spot - shift[axis].astype(F32)
            spots.append(spot)
        value = jnp.concatenate(spots + new_vel + new_aff + [new_vol], 0)
        out[:, lanes] = jnp.where(moving == 4, value, 0.0)
        high = value.astype(BF16)
        rest = value - high.astype(F32)
        middle = rest.astype(BF16)
        low = (rest - middle.astype(F32)).astype(BF16)
        parts = jnp.concatenate([high, middle, low], 0)
        packed[...] += lax.dot_general(parts, chosen[:, lanes], NT, preferred_element_type=F32)

    loop(first)
    await_peers(counts)
    send_margins(0)
    loop(first_inner)
    add_margins(0)
    velocities()
    send_halo(0)
    fill_wide()
    loop(lambda step: gather_inner(0, step))
    rank_rows()
    fill_wide_edge(0)
    edge_total[...] = jnp.zeros_like(edge_total)
    total[...] = jnp.zeros_like(total)
    loop(second)
    send_margins(1)
    loop(second_inner)
    add_margins(1)
    velocities()
    send_halo(1)
    fill_wide()
    loop(lambda step: gather_inner(1, step))
    packed[...] = jnp.zeros_like(packed)
    fill_wide_edge(1)
    loop(last)
    for k in range(8):
        lanes = slice(k * capacity, (k + 1) * capacity)
        buckets[k] = packed[0:16, lanes] + packed[16:32, lanes] + packed[32:48, lanes]
    start_all(bucket_copies)
    wait_arrivals(bucket_copies)
    for k in range(8):
        out[:, sz.rows + k * capacity : sz.rows + (k + 1) * capacity] = arrived[k]
    for copies in margin_copies + halo_copies + [bucket_copies]:
        wait_sends(copies)


def vmem(count):
    return [pl.BlockSpec(memory_space=pltpu.VMEM)] * count


def per_device(counts, base, offset, velocity, affine, volume, node_mask, direction):
    size_x, size_y, depth = node_mask.shape
    rows = velocity.shape[1]
    capacity = rows // 16
    sz = Sizes(size_x, size_y, depth, rows, min(rows, 512))
    base = jnp.swapaxes(base, 0, 1)
    offset = jnp.swapaxes(offset, 0, 1)
    volume = volume.reshape(1, rows)
    direction = direction.reshape(1, rows)
    mask = node_mask.reshape(sz.cells, depth)
    width = sz.chunk
    scratch = [
        pltpu.VMEM((2, sz.steps, sz.edge + sz.cells, 3 * width), BF16),
        pltpu.VMEM((sz.steps, 4 * depth, 3 * width), BF16),
        pltpu.VMEM((2, depth, rows), F32),
        pltpu.VMEM((2, depth, rows), F32),
        pltpu.VMEM((3 * depth, 3 * width), F32),
        pltpu.VMEM((12, 8, rows), F32),
        pltpu.VMEM((sz.used, 4 * depth), F32),
        pltpu.VMEM((4, sz.cells, depth), F32),
        pltpu.VMEM((3, sz.cells, depth), F32),
        pltpu.VMEM((sz.cells, depth), F32),
        pltpu.VMEM((3 * depth, sz.cells), BF16),
        pltpu.VMEM((3 * depth, sz.edge), BF16),
        pltpu.VMEM((1, rows), F32),
        pltpu.VMEM((8 * capacity, rows), BF16),
        pltpu.VMEM((1, rows), jnp.int32),
        pltpu.VMEM((48, 8 * capacity), F32),
        pltpu.VMEM((size_x + 8, width), F32),
        pltpu.VMEM((size_x + 8, width), F32),
        pltpu.VMEM((size_y + 8, width), F32),
        pltpu.VMEM((size_y + 8, width), F32),
    ]
    for lanes in (4 * depth, 4 * depth, 3 * depth, 3 * depth):
        scratch.append(pltpu.VMEM((2, sz.corner, lanes), BF16))
        scratch.append(pltpu.VMEM((2, 4 * CORNER_ROWS, depth), BF16))
    scratch += [
        pltpu.VMEM((4 * CORNER_ROWS, depth), F32),
        pltpu.VMEM((8, 16, capacity), F32),
        pltpu.VMEM((8, 16, capacity), F32),
        pltpu.SemaphoreType.DMA((4, 8)),
        pltpu.SemaphoreType.DMA((4, 8)),
        pltpu.SemaphoreType.DMA((8,)),
        pltpu.SemaphoreType.DMA((8,)),
    ]
    return pl.pallas_call(
        functools.partial(kernel, sz, counts, capacity),
        out_shape=jax.ShapeDtypeStruct((16, rows + 8 * capacity), F32),
        in_specs=vmem(7),
        out_specs=vmem(1)[0],
        scratch_shapes=scratch,
        compiler_params=pltpu.CompilerParams(
            collective_id=0, has_side_effects=True, vmem_limit_bytes=60 * 1024 * 1024
        ),
        name="substeps",
    )(base, offset, velocity, affine, volume, mask, direction)


def solution(mesh):
    counts = (mesh.shape["gx"], mesh.shape["gy"])
    placed = (
        P(None, None, ("gx", "gy")),
        P(None, None, ("gx", "gy")),
        P(None, ("gx", "gy")),
        P(None, ("gx", "gy")),
        P(("gx", "gy")),
        P("gx", "gy", None),
        P(("gx", "gy")),
    )
    return jax.shard_map(
        functools.partial(per_device, counts),
        mesh=mesh,
        in_specs=placed,
        out_specs=P(None, ("gx", "gy")),
        check_vma=False,
    )
```

```python
import functools

import jax
import jax.numpy as jnp
from jax import lax
from jax.experimental import pallas as pl
from jax.experimental.pallas import tpu as pltpu
from jax.sharding import PartitionSpec as P

PARTICLE_MASS = 1.0
STIFFNESS = 4.0
TIME_STEP = 0.1
GRAVITY = 3.0
MASS_FLOOR = 0.5
LANES = 128
OUTSIDE = -100

F32 = jnp.float32
BF16 = jnp.bfloat16
NT = (((1,), (1,)), ((), ()))

SIDES = ((0, -1), (0, 1), (-1, 0), (1, 0))
CORNERS = ((-1, -1), (-1, 1), (1, -1), (1, 1))
BLOCKS = SIDES + CORNERS
ISSUE = (4, 5, 6, 7, 0, 1, 2, 3)
CORNER_ROWS = 16
UNROLL = (False,) * 7


class Sizes:
    def __init__(self, size_x, size_y, depth, rows, chunk):
        self.x, self.y, self.depth, self.rows, self.chunk = size_x, size_y, depth, rows, chunk
        self.steps = rows // chunk
        self.cells = size_x * size_y
        counts = [2 * size_x] * 2 + [2 * size_y] * 2
        self.sides = [(sum(counts[:k]), counts[k]) for k in range(4)]
        self.corner = sum(counts)
        self.used = self.corner + 16
        self.edge = self.used


def spline(frac):
    return [0.5 * (1.5 - frac) ** 2, 0.75 - (frac - 1.0) ** 2, 0.5 * (frac - 0.5) ** 2]


def pick(place, values):
    return jnp.where(
        place == 0,
        values[0],
        jnp.where(place == 1, values[1], jnp.where(place == 2, values[2], 0.0)),
    )


def weights_of(offsets):
    weights = spline(offsets)
    return (weights, [weights[node] * (float(node) - offsets) for node in range(3)])


def rows_iota(count):
    return lax.broadcasted_iota(jnp.int32, (count, 1), 0)


def groups(width):
    return [slice(low, low + LANES) for low in range(0, width, LANES)]


def put(tab, width, group, row, count, wx, sx, wy, sy):
    for third, value in enumerate((wx * wy, sx * wy, wx * sy)):
        low = third * width + group.start
        tab[row : row + count, low : low + LANES] = value.astype(BF16)


def build_edge(sz, bases, offsets, tab, tables):
    all_weights, all_slopes = weights_of(offsets)
    edge = rows_iota(8)
    for group in groups(sz.chunk):
        weights = [[value[axis : axis + 1, group] for value in all_weights] for axis in range(3)]
        slopes = [[value[axis : axis + 1, group] for value in all_slopes] for axis in range(3)]
        from_x = bases[0:1, group] + 2
        from_y = bases[1:2, group] + 2
        pairs = []
        for size, start, axis in ((sz.x, from_x, 0), (sz.y, from_y, 1)):
            place = rows_iota(size) + 2 - start
            plain, slope = (pick(place, weights[axis]), pick(place, slopes[axis]))
            tables[2 * axis][0:size, group] = plain
            tables[2 * axis + 1][0:size, group] = slope
            place = jnp.where(edge < 2, edge, jnp.where(edge < 4, edge + size, OUTSIDE)) - start
            pairs.append((plain, slope, pick(place, weights[axis]), pick(place, slopes[axis])))
        wide_w, wide_s, out_xw, out_xs = pairs[0]
        tall_w, tall_s, out_yw, out_ys = pairs[1]
        for k in range(4):
            one = slice(k, k + 1)
            put(tab, sz.chunk, group, k * sz.x, sz.x, wide_w, wide_s, out_yw[one], out_ys[one])
        for k in range(4):
            one = slice(k, k + 1)
            row = sz.sides[2][0] + k * sz.y
            put(tab, sz.chunk, group, row, sz.y, out_xw[one], out_xs[one], tall_w, tall_s)
        spot = rows_iota(16)
        place_x = ((spot >> 1) & 1) + (spot >> 3) * (sz.x + 2) - from_x
        place_y = (spot & 1) + ((spot >> 2) & 1) * (sz.y + 2) - from_y
        put(
            tab, sz.chunk, group, sz.corner, 16, pick(place_x, weights[0]), pick(place_x, slopes[0]),
            pick(place_y, weights[1]), pick(place_y, slopes[1]),
        )


def build_depth(sz, bases, offsets, depth_w, depth_s):
    all_weights, all_slopes = weights_of(offsets[2:3])
    for group in groups(sz.chunk):
        place = rows_iota(sz.depth) - bases[2:3, group]
        depth_w[:, group] = pick(place, [value[:, group] for value in all_weights])
        depth_s[:, group] = pick(place, [value[:, group] for value in all_slopes])


def build_inner(sz, tab, tables):
    xw, xs, yw, ys = tables
    for group in groups(sz.chunk):
        wide_w, wide_s = (xw[0 : sz.x, group], xs[0 : sz.x, group])
        for y in range(sz.y):
            one = slice(y, y + 1)
            put(
                tab, sz.chunk, group, sz.edge + y * sz.x, sz.x, wide_w, wide_s,
                yw[one, group], ys[one, group],
            )


def build_right(sz, vel, aff, vol, depth_w, depth_s, right):
    depth = sz.depth
    width = sz.chunk
    all_stress = -STIFFNESS * (vol - 1.0)
    for group in groups(width):
        stress = all_stress[:, group]

        def entry(i, j):
            value = PARTICLE_MASS * aff[3 * i + j][:, group]
            return value + stress if i == j else value

        def store(third, rows, value):
            low = third * width + group.start
            right[rows, low : low + LANES] = value.astype(BF16)

        plain = depth_w[:, group]
        slope = depth_s[:, group]
        store(0, slice(0, depth), plain * PARTICLE_MASS)
        for i in range(3):
            rows = slice((i + 1) * depth, (i + 2) * depth)
            moment = PARTICLE_MASS * vel[i][:, group]
            store(0, rows, plain * moment + slope * entry(i, 2))
            store(1, rows, plain * entry(i, 0))
            store(2, rows, plain * entry(i, 1))


def reduce_depth(sz, result, depth_w, depth_s):
    parts = []

    def fold(value):
        return jnp.sum(value.reshape(sz.depth // 8, 8, LANES), 0)

    for group in groups(sz.chunk):
        weight, slope = (depth_w[:, group], depth_s[:, group])
        sums = []
        for i in range(3):
            rows = slice(i * sz.depth, (i + 1) * sz.depth)
            thirds = [
                result[rows, third * sz.chunk + group.start : third * sz.chunk + group.stop]
                for third in range(3)
            ]
            sums += [fold(third * weight) for third in thirds] + [fold(thirds[0] * slope)]
        parts.append(sums)
    return [jnp.concatenate([sums[k] for sums in parts], 1) for k in range(12)]


def finish(sums, vol):
    vel = [jnp.sum(sums[4 * i], 0, keepdims=True) for i in range(3)]
    aff = [
        4.0 * jnp.sum(sums[4 * i + 1 + a], 0, keepdims=True) for i in range(3) for a in range(3)
    ]
    return (vel, aff, vol * (1.0 + TIME_STEP * (aff[0] + aff[4] + aff[8])))


def neighbour(counts, dx, dy):
    to_x = lax.axis_index("gx") + dx
    to_y = lax.axis_index("gy") + dy
    exists = (to_x >= 0) & (to_x < counts[0]) & (to_y >= 0) & (to_y < counts[1])
    return (exists, {"gx": to_x, "gy": to_y})


def greet(counts):
    barrier = pltpu.get_barrier_semaphore()
    for dx, dy in BLOCKS:
        exists, where = neighbour(counts, dx, dy)

        @pl.when(exists)
        def _():
            pl.semaphore_signal(
                barrier, inc=1, device_id=where, device_id_type=pl.DeviceIdType.MESH
            )


def await_peers(counts):
    barrier = pltpu.get_barrier_semaphore()
    peers = 0
    for dx, dy in BLOCKS:
        exists, _ = neighbour(counts, dx, dy)
        peers = peers + exists.astype(jnp.int32)
    pl.semaphore_wait(barrier, peers)


def transfers(counts, sign, source, target, send_sems, recv_sems):
    copies = []
    for k, (dx, dy) in enumerate(BLOCKS):
        exists, where = neighbour(counts, sign * dx, sign * dy)
        copy = pltpu.make_async_remote_copy(
            src_ref=source(k),
            dst_ref=target(k),
            send_sem=send_sems.at[k],
            recv_sem=recv_sems.at[k],
            device_id=where,
            device_id_type=pl.DeviceIdType.MESH,
        )
        comes, _ = neighbour(counts, -sign * dx, -sign * dy)
        copies.append((exists, comes, copy))
    return copies


def start_all(copies, picked=ISSUE):
    for k in picked:
        pl.when(copies[k][0])(copies[k][2].start)


def wait_arrivals(copies, picked=ISSUE):
    for k in picked:
        pl.when(copies[k][1])(copies[k][2].wait_recv)


def wait_sends(copies):
    for exists, _, copy in copies:
        pl.when(exists)(copy.wait_send)


def clear_missing(counts, sign, target):
    for k, (dx, dy) in enumerate(BLOCKS):
        comes, _ = neighbour(counts, -sign * dx, -sign * dy)

        @pl.when(jnp.logical_not(comes))
        def _():
            view = target(k)
            view[...] = jnp.zeros(view.shape, view.dtype)


def edge_views(sz, sides, tiles):
    def view(k):
        if k < 4:
            return sides.at[pl.ds(*sz.sides[k])]
        return tiles.at[pl.ds((k - 4) * CORNER_ROWS, CORNER_ROWS)]

    return view


def kernel(sz, counts, capacity, *refs):
    held, placed, out, scratch = (refs[:7], refs[7], refs[15], refs[16:])
    base, offset, vel, aff, vol, mask, direction = refs[8:15]
    loads = [
        pltpu.make_async_copy(held[k], refs[8 + k], scratch[-1].at[k]) for k in range(7)
    ]
    for load in loads:
        load.start()
    (
        tabs, right, depth_w, depth_s, result, inner_sums, edge_total, total, speed, keep, wide, wide_edge,
        ratio, chosen, hits, masked, packed, xw, xs, yw, ys,
        margins, corners, got, got_corners, sent, sent_corners, halo, halo_corners, spread,
        buckets, nothing, send_sems, recv_sems, bucket_sends, bucket_recvs,
    ) = scratch[:-1]
    size_x, size_y, depth = sz.x, sz.y, sz.depth
    width = sz.chunk
    greet(counts)

    margin_copies, halo_copies = ([], [])
    for s in range(2):
        arriving = edge_views(sz, got.at[s], got_corners.at[s])
        margin_copies.append(
            transfers(
                counts, 1, edge_views(sz, margins.at[s], corners.at[s]), arriving,
                send_sems.at[2 * s], recv_sems.at[2 * s],
            )
        )
        arriving = edge_views(sz, halo.at[s], halo_corners.at[s])
        halo_copies.append(
            transfers(
                counts, -1, edge_views(sz, sent.at[s], sent_corners.at[s]), arriving,
                send_sems.at[2 * s + 1], recv_sems.at[2 * s + 1],
            )
        )
    order = [0, 1, 2, 3, 5, 6, 7, 8]
    slot_of = [order.index(3 * (dx + 1) + dy + 1) for dx, dy in BLOCKS]

    def bucket_place(k):
        return placed.at[:, pl.ds(sz.rows + slot_of[k] * capacity, capacity)]

    bucket_copies = transfers(
        counts, 1, lambda k: buckets.at[slot_of[k]], bucket_place, bucket_sends, bucket_recvs
    )
    clears = []
    for k in range(8):
        clear_copy = pltpu.make_async_copy(nothing, bucket_place(k), scratch[-1].at[8 + k])
        clears.append((jnp.logical_not(bucket_copies[k][1]), clear_copy))
    def lanes_of(step):
        if isinstance(step, int):
            return slice(step * width, (step + 1) * width)
        return pl.ds(pl.multiple_of(step * width, width), width)

    def clear():
        for s in range(2):
            clear_missing(counts, 1, edge_views(sz, got.at[s], got_corners.at[s]))
            clear_missing(counts, -1, edge_views(sz, halo.at[s], halo_corners.at[s]))
        nothing[...] = jnp.zeros_like(nothing)
        for missing, clear_copy in clears:
            pl.when(missing)(clear_copy.start)
        loads[5].wait()
        for y in range(size_y):
            column = mask[pl.ds(y, size_x, stride=size_y), :]
            keep[y * size_x : (y + 1) * size_x] = (1 - column).astype(F32)

    def tables_of(step):
        return [table.at[step] for table in (xw, xs, yw, ys)]

    def prepare(s, step):
        lanes = lanes_of(step)
        build_edge(sz, base[:, s, lanes], offset[:, s, lanes], tabs.at[s, step], tables_of(step))

    def prepare_depth(s, step):
        lanes = lanes_of(step)
        build_depth(
            sz, base[:, s, lanes], offset[:, s, lanes],
            depth_w.at[s, :, lanes], depth_s.at[s, :, lanes],
        )

    def scatter_edge(s, step):
        edge_total[...] += lax.dot_general(
            tabs[s, step, 0 : sz.used], right[step], NT, preferred_element_type=F32
        )

    def scatter_inner(s, step):
        added = lax.dot_general(
            tabs[s, step, sz.edge :], right[step], NT, preferred_element_type=F32
        )
        for c in range(4):
            total[c] += added[:, c * depth : (c + 1) * depth]

    def send_margins(s):
        margins[s] = edge_total[0 : sz.corner].astype(BF16)
        for k in range(4):
            for c in range(4):
                spread[k * 16 + 4 * c : k * 16 + 4 * c + 4, :] = edge_total[
                    sz.corner + 4 * k : sz.corner + 4 * k + 4, c * depth : (c + 1) * depth
                ]
        corners[s] = spread[...].astype(BF16)
        start_all(margin_copies[s])

    def add_margins(s):
        wait_arrivals(margin_copies[s])
        for k, low in ((1, 0), (0, sz.cells - 2 * size_x)):
            start, count = sz.sides[k]
            for c in range(4):
                block = got[s, start : start + count, c * depth : (c + 1) * depth]
                total[c, low : low + count] += block.astype(F32)
        for k, low in ((2, size_x - 2), (3, 0)):
            start = sz.sides[k][0]
            block = got[s, start : start + 2 * size_y].astype(F32)
            for i in range(2):
                rows = pl.ds(low + i, size_y, stride=size_x)
                for c in range(4):
                    lanes = slice(c * depth, (c + 1) * depth)
                    total[c, rows] += block[i * size_y : (i + 1) * size_y, lanes]
        spread[...] = got_corners[s].astype(F32)
        for k, (dx, dy) in enumerate(CORNERS):
            low_x = size_x - 2 if dx < 0 else 0
            low_y = size_y - 2 if dy < 0 else 0
            for i in range(2):
                for j in range(2):
                    row = (low_y + j) * size_x + low_x + i
                    for c in range(4):
                        here = k * 16 + 4 * c + 2 * i + j
                        total[c, row : row + 1] += spread[here : here + 1]

    def velocities(low, count):
        rows = slice(low, low + count)
        mass = jnp.maximum(total[0, rows], MASS_FLOOR)
        for axis in range(3):
            value = total[axis + 1, rows] / mass
            if axis == 2:
                value = value - TIME_STEP * GRAVITY
            speed[axis, rows] = value * keep[rows]

    def send_halo(s):
        border = 2 * size_x
        for k, low in ((1, 0), (0, sz.cells - border)):
            velocities(low, border)
            start, count = sz.sides[k]
            for c in range(3):
                lanes = slice(c * depth, (c + 1) * depth)
                sent[s, start : start + count, lanes] = speed[c, low : low + count].astype(BF16)
        for k, (dx, dy) in enumerate(CORNERS):
            low_x = size_x - 2 if dx < 0 else 0
            low_y = size_y - 2 if dy < 0 else 0
            for i in range(2):
                for j in range(2):
                    row = (low_y + j) * size_x + low_x + i
                    for c in range(3):
                        here = k * 16 + 4 * c + 2 * i + j
                        spread[here : here + 1] = speed[c, row : row + 1]
        sent_corners[s] = spread[...].astype(BF16)
        start_all(halo_copies[s], ISSUE[:6])
        velocities(border, sz.cells - 2 * border)
        for k, low in ((2, size_x - 2), (3, 0)):
            for i in range(2):
                start = sz.sides[k][0] + i * size_y
                rows = pl.ds(low + i, size_y, stride=size_x)
                for c in range(3):
                    lanes = slice(c * depth, (c + 1) * depth)
                    sent[s, start : start + size_y, lanes] = speed[c, rows].astype(BF16)
        start_all(halo_copies[s], ISSUE[6:])

    def fill_wide():
        for c in range(3):
            wide[c * depth : (c + 1) * depth, :] = speed[c].T.astype(BF16)

    def fill_wide_edge(s):
        wait_arrivals(halo_copies[s])
        spread[...] = halo_corners[s].astype(F32)
        for c in range(3):
            lanes = slice(c * depth, (c + 1) * depth)
            tiles = [spread[k * 16 + 4 * c : k * 16 + 4 * c + 4] for k in range(4)]
            outer = jnp.concatenate([halo[s, :, lanes].astype(F32)] + tiles, 0)
            wide_edge[lanes, :] = outer.T.astype(BF16)

    def gather_inner(s, step):
        lanes = lanes_of(step)
        here = result.at[step % 2]
        here[...] = jnp.dot(wide[...], tabs[s, step, sz.edge :], preferred_element_type=F32)
        sums = reduce_depth(sz, here, depth_w.at[s, :, lanes], depth_s.at[s, :, lanes])
        for k in range(12):
            inner_sums[k, :, lanes] = sums[k]

    def gather_edge(s, step, volume):
        lanes = lanes_of(step)
        here = result.at[step % 2]
        here[...] = jnp.dot(wide_edge[...], tabs[s, step, 0 : sz.edge], preferred_element_type=F32)
        sums = reduce_depth(sz, here, depth_w.at[s, :, lanes], depth_s.at[s, :, lanes])
        return finish([sums[k] + inner_sums[k, :, lanes] for k in range(12)], volume)

    def loop(body, unrolled):
        if unrolled:
            for step in range(sz.steps):
                body(step)
        else:
            lax.fori_loop(0, sz.steps, lambda step, carry: (body(step), carry)[1], 0)

    def rows_of(ref, lanes, count):
        return [ref[k : k + 1, lanes] for k in range(count)]

    def first(step):
        lanes = lanes_of(step)
        right[step, 0:depth, width : 3 * width] = jnp.zeros((depth, 2 * width), BF16)
        prepare(0, step)
        prepare_depth(0, step)
        build_right(
            sz, rows_of(vel, lanes, 3), rows_of(aff, lanes, 9), vol[:, lanes],
            depth_w.at[0, :, lanes], depth_s.at[0, :, lanes], right.at[step],
        )
        scatter_edge(0, step)

    def first_inner(step):
        build_inner(sz, tabs.at[0, step], tables_of(step))
        scatter_inner(0, step)
        prepare_depth(1, step)

    def first_gather(step):
        gather_inner(0, step)
        prepare(1, step)

    def second(step):
        lanes = lanes_of(step)
        new_vel, new_aff, new_vol = gather_edge(0, step, vol[:, lanes])
        ratio[:, lanes] = new_vol
        build_right(
            sz, new_vel, new_aff, new_vol, depth_w.at[1, :, lanes], depth_s.at[1, :, lanes],
            right.at[step],
        )
        scatter_edge(1, step)

    index_x = lax.axis_index("gx")
    index_y = lax.axis_index("gy")

    def route(code):
        step_x = jnp.where(code < 3, -1, jnp.where(code > 5, 1, 0))
        step_y = code - 3 * step_x - 4
        to_x = step_x + index_x
        to_y = step_y + index_y
        inside = (to_x >= 0) & (to_x < counts[0]) & (to_y >= 0) & (to_y < counts[1])
        return (
            jnp.where(inside, code, 4),
            jnp.where(inside, step_x, 0),
            jnp.where(inside, step_y, 0),
        )

    def rank_rows():
        parts = sz.rows // LANES
        place = rows_iota(8)
        codes = jnp.where(place < 4, place, place + 1)
        marks = []
        for part in range(parts):
            moving, _, _ = route(direction[:, part * LANES : (part + 1) * LANES])
            marks.append(jnp.where(moving == codes, 1.0, 0.0))
        above = lax.broadcasted_iota(jnp.int32, (LANES, 2 * LANES), 0)
        along = lax.broadcasted_iota(jnp.int32, (LANES, 2 * LANES), 1)
        summer = jnp.where(above <= along, 1.0, 0.0).astype(BF16)
        sums = jnp.dot(
            jnp.concatenate(marks, 0).astype(BF16), summer, preferred_element_type=F32
        )
        before = jnp.zeros((8, LANES), F32)
        for part in range(parts):
            mine = slice(part * 8, (part + 1) * 8)
            lanes = slice(part * LANES, (part + 1) * LANES)
            rank = jnp.sum(marks[part] * (sums[mine, 0:LANES] + before), 0, keepdims=True) - 1.0
            here = rank.astype(jnp.int32) == rows_iota(capacity)
            chosen[:, lanes] = jnp.where(here, 1.0, 0.0).astype(BF16)
            hits[:, lanes] = marks[part]
            before = before + sums[mine, LANES:]

    def second_inner(step):
        build_inner(sz, tabs.at[1, step], tables_of(step))
        scatter_inner(1, step)

    def last(step):
        lanes = lanes_of(step)
        new_vel, new_aff, new_vol = gather_edge(1, step, ratio[:, lanes])
        moving, step_x, step_y = route(direction[:, lanes])
        shift = (step_x * size_x, step_y * size_y, None)
        bases = base[:, 1, lanes]
        offsets = offset[:, 1, lanes]
        spots = []
        for axis in range(3):
            spot = bases[axis : axis + 1].astype(F32) + offsets[axis : axis + 1]
            spot = spot + TIME_STEP * new_vel[axis]
            if shift[axis] is not None:
                spot = spot - shift[axis].astype(F32)
            spots.append(spot)
        value = jnp.concatenate(spots + new_vel + new_aff + [new_vol], 0)
        out[:, lanes] = jnp.where(moving == 4, value, 0.0)
        high = value.astype(BF16).astype(F32)
        rest = value - high
        middle = rest.astype(BF16).astype(F32)
        for part, piece in enumerate((high, middle, rest - middle)):
            for k in range(8):
                row = (3 * k + part) * 16
                masked[step % 2, row : row + 16] = (piece * hits[k : k + 1, lanes]).astype(BF16)
        packed[...] += lax.dot_general(
            masked[step % 2], chosen[:, lanes], NT, preferred_element_type=F32
        )

    edge_total[...] = jnp.zeros_like(edge_total)
    for load in loads[:5]:
        load.wait()
    loop(first, UNROLL[0])
    await_peers(counts)
    send_margins(0)
    clear()
    total[...] = jnp.zeros_like(total)
    loop(first_inner, UNROLL[1])
    add_margins(0)
    send_halo(0)
    fill_wide()
    loop(first_gather, UNROLL[2])
    loads[6].wait()
    rank_rows()
    edge_total[...] = jnp.zeros_like(edge_total)
    fill_wide_edge(0)
    loop(second, UNROLL[3])
    send_margins(1)
    total[...] = jnp.zeros_like(total)
    loop(second_inner, UNROLL[4])
    add_margins(1)
    send_halo(1)
    fill_wide()
    loop(lambda step: gather_inner(1, step), UNROLL[5])
    packed[...] = jnp.zeros_like(packed)
    fill_wide_edge(1)
    loop(last, UNROLL[6])
    for k in range(8):
        rows = [slice((3 * k + part) * 16, (3 * k + part + 1) * 16) for part in range(3)]
        buckets[k] = packed[rows[0]] + packed[rows[1]] + packed[rows[2]]
    start_all(bucket_copies)
    store = pltpu.make_async_copy(out, placed.at[:, pl.ds(0, sz.rows)], scratch[-1].at[7])
    store.start()
    wait_arrivals(bucket_copies)
    for copies in margin_copies + halo_copies + [bucket_copies]:
        wait_sends(copies)
    for missing, clear_copy in clears:
        pl.when(missing)(clear_copy.wait)
    store.wait()


def per_device(counts, base, offset, velocity, affine, volume, node_mask, direction):
    size_x, size_y, depth = node_mask.shape
    rows = velocity.shape[1]
    capacity = rows // 16
    sz = Sizes(size_x, size_y, depth, rows, min(rows, 1024))
    base = jnp.swapaxes(base, 0, 1)
    offset = jnp.swapaxes(offset, 0, 1)
    volume = volume.reshape(1, rows)
    direction = direction.reshape(1, rows)
    mask = node_mask.reshape(sz.cells, depth)
    width = sz.chunk
    scratch = [pltpu.VMEM(x.shape, x.dtype) for x in (base, offset, velocity, affine, volume, mask, direction)]
    scratch += [
        pltpu.VMEM((16, rows), F32),
        pltpu.VMEM((2, sz.steps, sz.edge + sz.cells, 3 * width), BF16),
        pltpu.VMEM((sz.steps, 4 * depth, 3 * width), BF16),
        pltpu.VMEM((2, depth, rows), F32),
        pltpu.VMEM((2, depth, rows), F32),
        pltpu.VMEM((2, 3 * depth, 3 * width), F32),
        pltpu.VMEM((12, 8, rows), F32),
        pltpu.VMEM((sz.used, 4 * depth), F32),
        pltpu.VMEM((4, sz.cells, depth), F32),
        pltpu.VMEM((3, sz.cells, depth), F32),
        pltpu.VMEM((sz.cells, depth), F32),
        pltpu.VMEM((3 * depth, sz.cells), BF16),
        pltpu.VMEM((3 * depth, sz.edge), BF16),
        pltpu.VMEM((1, rows), F32),
        pltpu.VMEM((capacity, rows), BF16),
        pltpu.VMEM((8, rows), F32),
        pltpu.VMEM((2, 8 * 48, width), BF16),
        pltpu.VMEM((8 * 48, capacity), F32),
        pltpu.VMEM((sz.steps, size_x, width), F32),
        pltpu.VMEM((sz.steps, size_x, width), F32),
        pltpu.VMEM((sz.steps, size_y, width), F32),
        pltpu.VMEM((sz.steps, size_y, width), F32),
    ]
    for lanes in (4 * depth, 4 * depth, 3 * depth, 3 * depth):
        scratch.append(pltpu.VMEM((2, sz.corner, lanes), BF16))
        scratch.append(pltpu.VMEM((2, 4 * CORNER_ROWS, depth), BF16))
    scratch += [
        pltpu.VMEM((4 * CORNER_ROWS, depth), F32),
        pltpu.VMEM((8, 16, capacity), F32),
        pltpu.VMEM((16, capacity), F32),
        pltpu.SemaphoreType.DMA((4, 8)),
        pltpu.SemaphoreType.DMA((4, 8)),
        pltpu.SemaphoreType.DMA((8,)),
        pltpu.SemaphoreType.DMA((8,)),
        pltpu.SemaphoreType.DMA((16,)),
    ]
    return pl.pallas_call(
        functools.partial(kernel, sz, counts, capacity),
        out_shape=jax.ShapeDtypeStruct((16, rows + 8 * capacity), F32),
        in_specs=[pl.BlockSpec(memory_space=pltpu.HBM)] * 7,
        out_specs=pl.BlockSpec(memory_space=pltpu.HBM),
        scratch_shapes=scratch,
        compiler_params=pltpu.CompilerParams(
            collective_id=0, has_side_effects=True, vmem_limit_bytes=60 * 1024 * 1024
        ),
        name="substeps",
    )(base, offset, velocity, affine, volume, mask, direction)


def solution(mesh):
    counts = (mesh.shape["gx"], mesh.shape["gy"])
    placed = (
        P(None, None, ("gx", "gy")),
        P(None, None, ("gx", "gy")),
        P(None, ("gx", "gy")),
        P(None, ("gx", "gy")),
        P(("gx", "gy")),
        P("gx", "gy", None),
        P(("gx", "gy")),
    )
    return jax.shard_map(
        functools.partial(per_device, counts),
        mesh=mesh,
        in_specs=placed,
        out_specs=P(None, ("gx", "gy")),
        check_vma=False,
    )
```
